256 devices in a mesh: dp: 64 (over z, y, core), col: 4 (over x).
Axes of the slice: x: 4, y: 4, z: 8, core: 2. Of those that a mesh axis runs over, the one named last changes fastest.
Arguments:
- view_first: bfloat16 [65536, 4096], P('dp'), may hold values from -1000 to 1000
- view_second: bfloat16 [65536, 4096], P('dp', 'col'), may hold values from -1000 to 1000
- valid_rows: int32 [64], P('dp'), may hold values from 1 to 1024, as said below
Outputs:
- correlation: float32 [4096, 4096], P('dp', 'col')
- loss: float32 [], replicated
The draws below stay inside these ranges and needn't reach their ends.
Inputs may be any that keep to these rules, and one draw needn't show every extreme that they name: `valid_rows`: some micro-batch uses all 1024 rows.
All inputs are finite; a program needn't handle non-finite values.
Results may differ from the reference program's by a relative error of at most 0.0005.
Values sent between devices are 32-bit elements; how exact they have to be, the bound alone decides.
No kernel may reach another device: no remote copies, remote signals or barrier semaphores. Data moves between devices by JAX's collectives and lax.ppermute only.
A program may use at most 128 MiB of HBM per device.

```python
import math
import jax
import jax.numpy as jnp
from jax import lax

D = 4096
TOK_DEV = 1024
GROUPS = 64
TOKENS = 65536


def paired_views(key):
    keys = jax.random.split(jax.random.fold_in(key, 11), 9)
    steps = jnp.arange(GROUPS, dtype=jnp.float32)
    rising = 1.0 + 2.0 * steps / max(GROUPS - 1, 1)
    shift_first = jnp.clip(jax.random.normal(keys[0], (GROUPS, D)), -6.0, 6.0) * 1.5 * rising[:, None]
    other_shift = jnp.clip(jax.random.normal(keys[1], (GROUPS, D)), -6.0, 6.0) * 1.5 * rising[:, None]
    shift_second = 0.7 * shift_first + 0.7 * other_shift
    scale_first = jnp.exp(jax.random.uniform(keys[2], (D,), minval=0.0, maxval=math.log(10.0)))
    scale_second = jnp.exp(jax.random.uniform(keys[3], (D,), minval=0.0, maxval=math.log(10.0)))
    base = jnp.clip(jax.random.normal(keys[5], (TOKENS, D)), -6.0, 6.0)
    noise = jnp.clip(jax.random.normal(keys[6], (TOKENS, D)), -6.0, 6.0)
    center_first = jnp.clip(jax.random.normal(keys[7], (D,)), -6.0, 6.0)
    center_second = jnp.clip(jax.random.normal(keys[8], (D,)), -6.0, 6.0)
    rows_first = jnp.repeat(shift_first, TOK_DEV, axis=0)
    rows_second = jnp.repeat(shift_second, TOK_DEV, axis=0)
    first = (base + rows_first + center_first[None, :]) * scale_first[None, :]
    second = (0.8 * base + 0.6 * noise + rows_second + center_second[None, :]) * scale_second[None, :]
    return (first, second)


def draw_view_first(key, part):
    return paired_views(key)[0].astype(jnp.bfloat16)


def draw_view_second(key, part):
    return paired_views(key)[1].astype(jnp.bfloat16)


def draw_valid_rows(key, part):
    steps = jnp.arange(GROUPS, dtype=jnp.int32)
    lowest = TOK_DEV // 3
    rising = lowest + (TOK_DEV - lowest) * steps // max(GROUPS - 1, 1)
    jitter = jax.random.randint(jax.random.fold_in(key, 5), (GROUPS,), -(TOK_DEV // 8), 1)
    counts = jnp.clip(rising + jitter, 1, TOK_DEV)
    full_group = jax.random.randint(jax.random.fold_in(key, 9), (), 0, GROUPS)
    return jnp.where(steps == full_group, TOK_DEV, counts).astype(jnp.int32)


def setup_inputs(seed: int = 0) -> dict:
    key_list = jax.random.split(jax.random.key(seed), 4)
    return {
        "view_first": draw_view_first(jax.random.fold_in(key_list[3], 71), 0),
        "view_second": draw_view_second(jax.random.fold_in(key_list[3], 71), 0),
        "valid_rows": draw_valid_rows(jax.random.fold_in(key_list[3], 71), 0),
    }


epsilon = 1e-05
off_weight = 0.0051

def centered_group(block, used_rows):
    positions = jnp.arange(TOK_DEV, dtype=jnp.int32)
    live_col = (positions < used_rows)[:, None].astype(jnp.float32)
    used_float = used_rows.astype(jnp.float32)
    totals = lax.optimization_barrier(jnp.sum(block.astype(jnp.float32) * live_col, axis=0))
    means = totals / used_float
    centered = ((block.astype(jnp.float32) - means) * live_col).astype(jnp.bfloat16)
    return (totals, means, centered)

def reference(view_first, view_second, valid_rows):
    first = view_first.reshape(GROUPS, TOK_DEV, D)
    second = view_second.reshape(GROUPS, TOK_DEV, D)

    def group_terms(inputs):
        block_first, block_second, used_rows = inputs
        sum_first, mean_first, cent_first = centered_group(block_first, used_rows)
        sum_second, mean_second, cent_second = centered_group(block_second, used_rows)
        square_first = lax.optimization_barrier(jnp.sum(jnp.square(cent_first.astype(jnp.float32)), axis=0))
        square_second = lax.optimization_barrier(jnp.sum(jnp.square(cent_second.astype(jnp.float32)), axis=0))
        return (sum_first, sum_second, mean_first, mean_second, square_first, square_second)
    sums_first, sums_second, means_first, means_second, squares_first, squares_second = lax.map(group_terms, (first, second, valid_rows))
    counts = valid_rows.astype(jnp.float32)
    all_rows = jnp.sum(counts)
    glob_first = lax.optimization_barrier(jnp.sum(sums_first, axis=0)) / all_rows
    glob_second = lax.optimization_barrier(jnp.sum(sums_second, axis=0)) / all_rows
    shifts_first = means_first - glob_first[None, :]
    shifts_second = means_second - glob_second[None, :]
    spread_first = lax.optimization_barrier(jnp.sum(squares_first + counts[:, None] * jnp.square(shifts_first), axis=0))
    spread_second = lax.optimization_barrier(jnp.sum(squares_second + counts[:, None] * jnp.square(shifts_second), axis=0))

    def accumulate(running, inputs):
        block_first, block_second, used_rows, shift_first, shift_second = inputs
        cent_first = centered_group(block_first, used_rows)[2]
        cent_second = centered_group(block_second, used_rows)[2]
        product = jnp.dot(cent_first.T, cent_second, preferred_element_type=jnp.float32)
        used_float = used_rows.astype(jnp.float32)
        return (running + product + used_float * shift_first[:, None] * shift_second[None, :], None)
    moment, unused = lax.scan(accumulate, jnp.zeros((D, D), jnp.float32), (first, second, valid_rows, shifts_first, shifts_second))
    scale_first = jnp.sqrt(spread_first / all_rows + epsilon)
    scale_second = jnp.sqrt(spread_second / all_rows + epsilon)
    correlation = moment / (all_rows * scale_first[:, None] * scale_second[None, :])
    index_rows = jnp.arange(D, dtype=jnp.int32)
    diagonal = index_rows[:, None] == index_rows[None, :]
    terms = jnp.where(diagonal, jnp.square(1.0 - correlation), off_weight * jnp.square(correlation))
    loss = jnp.sum(terms) / D
    return (correlation, loss)
```

```python
import functools

import jax
import jax.numpy as jnp
from jax import lax
from jax.experimental import pallas as pl
from jax.experimental.pallas import tpu as pltpu
from jax.sharding import Mesh
from jax.sharding import PartitionSpec as P


F32 = jnp.float32
BF16 = jnp.bfloat16
EPS = 1e-05
OFF = 0.0051

ROWS = 1024
FEAT = 4096
COLS = 1024
CA = 640
CB = COLS - CA
TILE = 512
ORDER = (4, 3, 5, 2, 6, 1, 7, 0)
AT = {d: i for i, d in enumerate(ORDER)}
CALLS = ((0, 1), (1, 3), (3, 8))
MB = -(-8 // (CB // 128))


def live_rows(n, rows, start):
    return lax.broadcasted_iota(jnp.int32, (rows, 1), 0) + start < n


def column_sums(n, x_ref):
    row = (lax.broadcasted_iota(jnp.int32, (8, ROWS), 1) < n).astype(F32).astype(BF16)
    return jnp.dot(row, x_ref[...], preferred_element_type=F32)[0:1]


def center(n, mean, x_ref, c_ref, width):
    step = 64

    def body(i, acc):
        at = pl.multiple_of(i * step, step)
        x = x_ref[pl.ds(at, step), :].astype(F32)
        c = jnp.where(live_rows(n, step, at), x - mean, 0.0).astype(BF16)
        c_ref[pl.ds(at, step), :] = c
        c = c.astype(F32)
        return acc + jnp.sum((c * c).reshape(step // 8, 8, width), axis=0)

    acc = lax.fori_loop(0, ROWS // step, body, jnp.zeros((8, width), F32))
    return jnp.sum(acc, axis=0, keepdims=True)


def second_kernel(tab, x_ref, c_ref, st_ref):
    n = tab[3]
    mean = column_sums(n, x_ref) / n.astype(F32)
    square = center(n, mean, x_ref, c_ref, x_ref.shape[1])
    width = x_ref.shape[1]
    st_ref[0:1, :] = mean
    st_ref[1:2, :] = square
    st_ref[2:3, :] = jnp.full((1, width), n.astype(F32))
    st_ref[3:8, :] = jnp.zeros((5, width), F32)


def second_view(tab, x):
    width = 512
    return pl.pallas_call(
        second_kernel,
        out_shape=(jax.ShapeDtypeStruct((ROWS, COLS), BF16), jax.ShapeDtypeStruct((8, COLS), F32)),
        grid_spec=pltpu.PrefetchScalarGridSpec(
            num_scalar_prefetch=1,
            grid=(COLS // width,),
            in_specs=[pl.BlockSpec((ROWS, width), lambda i, tab: (0, i))],
            out_specs=[
                pl.BlockSpec((ROWS, width), lambda i, tab: (0, i)),
                pl.BlockSpec((8, width), lambda i, tab: (0, i)),
            ],
        ),
        name="second_view",
    )(tab, x)


def tile_kernel(tab, x_ref, c2_ref, own_a, oth_a, own_b, oth_b, c1, prod):
    y, k, n = tab[1], tab[2], tab[3]
    mean = column_sums(n, x_ref) / n.astype(F32)
    square = center(n, mean, x_ref, c1, TILE)
    prod[0:TILE, :] = lax.dot_general(
        c1[...], c2_ref[...], (((0,), (0,)), ((), ())), preferred_element_type=F32
    )
    stats = jnp.concatenate([mean, square, jnp.zeros((6, TILE), F32)], axis=0)
    prod[TILE : TILE + 8, 0:TILE] = stats
    for dy in range(4):
        base = (y + dy) % 4 * 128
        for ra, rb, kk in ((own_a, own_b, k), (oth_a, oth_b, 1 - k)):
            at = pl.multiple_of(base + kk * 64, 64)
            ra[0, dy * 64 : dy * 64 + 64, :] = prod[pl.ds(at, 64), 0:CA]
            rb[0, dy] = prod[pl.ds(at, 64), CA:COLS]
        lanes = prod[TILE : TILE + 8, pl.ds(pl.multiple_of(base, 128), 128)]
        own_a[0, 256:264, dy * 128 : dy * 128 + 128] = lanes
        oth_a[0, 256:264, dy * 128 : dy * 128 + 128] = lanes
    own_a[0, 256:264, 512:CA] = jnp.zeros((8, CA - 512), F32)
    oth_a[0, 256:264, 512:CA] = jnp.zeros((8, CA - 512), F32)


def tiles(tab, x, c2, first, last):
    count = last - first
    a = jax.ShapeDtypeStruct((count, 264, CA), F32)
    b = jax.ShapeDtypeStruct((count, 4, 64, CB), F32)
    a_spec = pl.BlockSpec((1, 264, CA), lambda i, tab: (i, 0, 0))
    b_spec = pl.BlockSpec((1, 4, 64, CB), lambda i, tab: (i, 0, 0, 0))
    return pl.pallas_call(
        tile_kernel,
        out_shape=(a, a, b, b),
        grid_spec=pltpu.PrefetchScalarGridSpec(
            num_scalar_prefetch=1,
            grid=(count,),
            in_specs=[
                pl.BlockSpec((ROWS, TILE), lambda i, tab: (0, tab[8 + first + i])),
                pl.BlockSpec((ROWS, COLS), lambda i, tab: (0, 0)),
            ],
            out_specs=[a_spec, a_spec, b_spec, b_spec],
            scratch_shapes=[pltpu.VMEM((ROWS, TILE), BF16), pltpu.VMEM((TILE + 8, COLS), F32)],
        ),
        compiler_params=pltpu.CompilerParams(vmem_limit_bytes=48 * 2**20),
        name=f"tiles_{first}",
    )(tab, x, c2)


def pair(na, nb):
    n = na + nb
    return n, na * nb / n, nb / n


def column_of(row, tr, k):
    tr[...] = jnp.broadcast_to(row, (128, 128)).T
    return tr[pl.ds(pl.multiple_of(k * 64, 64), 64), 0:1]


class Stats:
    def __init__(self, n, m1, s1, m2, s2):
        self.n, self.m1, self.s1, self.m2, self.s2 = n, m1, s1, m2, s2


def merge_stats(a, b):
    n, w, f = pair(a.n, b.n)
    d1 = [q - p for p, q in zip(a.m1, b.m1)]
    d2 = b.m2 - a.m2
    m1 = [p + f * d for p, d in zip(a.m1, d1)]
    s1 = None if a.s1 is None else [p + q + w * d * d for p, q, d in zip(a.s1, b.s1, d1)]
    m2 = a.m2 + f * d2
    s2 = a.s2 + b.s2 + w * d2 * d2
    return Stats(n, m1, s1, m2, s2), [w * d for d in d1], d2


def lanes(ref, row, i):
    return ref[row : row + 1, i * 128 : i * 128 + 128]


def small_stats(ref):
    return Stats(
        ref[68:69, 0:1], [ref[64:65, 0:128]], [ref[65:66, 0:128]], ref[66:67, :], ref[67:68, :]
    )


def put_small(ref, s, width):
    ref[64:72, :] = jnp.zeros((8, width), F32)
    ref[64:65, 0:128] = s.m1[0]
    if s.s1 is not None:
        ref[65:66, 0:128] = s.s1[0]
    ref[66:67, :] = s.m2
    ref[67:68, :] = s.s2
    ref[68:69, :] = jnp.broadcast_to(s.n, (1, width))


def z_stats(ref, base, g, count):
    return Stats(
        ref[base + 6 : base + 7, g * 128 : g * 128 + 1],
        [lanes(ref, base, 2 * g + j) for j in range(2)],
        [lanes(ref, base + 1, 2 * g + j) for j in range(2)],
        ref[base + 2 + g : base + 3 + g, :],
        ref[base + 4 + g : base + 5 + g, :],
    )


def put_z_stats(ref, base, g, s):
    for j in range(2):
        at = (2 * g + j) * 128
        ref[base : base + 1, at : at + 128] = s.m1[j]
        ref[base + 1 : base + 2, at : at + 128] = s.s1[j]
    ref[base + 2 + g : base + 3 + g, :] = s.m2
    ref[base + 4 + g : base + 5 + g, :] = s.s2
    ref[base + 6 : base + 7, g * 128 : g * 128 + 128] = jnp.broadcast_to(s.n, (1, 128))


def a_local(own, peer, st, pst, g):
    return [
        Stats(
            s[2:3, 0:1],
            [lanes(p, 256, 2 * g + j) for j in range(2)],
            [lanes(p, 257, 2 * g + j) for j in range(2)],
            s[0:1, 0:CA],
            s[1:2, 0:CA],
        )
        for p, s in ((own, st), (peer, pst))
    ]


def a_kernel(plan, tab, own, peer, st, pst, *rest):
    received, outs, tr = rest[: plan["in"]], rest[plan["in"] : -1], rest[-1]
    k = tab[2]
    own, peer = own.at[0], peer.at[0]
    for o in outs:
        if len(o.shape) == 2:
            base = o.shape[0] - 8
            o[base : base + 8, :] = jnp.zeros((8, CA), F32)
    for g, (froms, out, row) in enumerate(plan["groups"]):
        mine, theirs = a_local(own, peer, st, pst, g)
        s, d1, d2 = merge_stats(mine, theirs)
        steps = [(d1, d2)]
        for r in froms:
            s, d1, d2 = merge_stats(s, z_stats(received[r], received[r].shape[0] - 8, g, 2))
            steps.append((d1, d2))
        o = outs[out]
        for j in range(2):
            at = (2 * g + j) * 64
            m = own[at : at + 64, :] + peer[at : at + 64, :]
            for r in froms:
                short = received[r].shape[0] == 136
                src = j * 64 if short else at
                m = m + received[r][src : src + 64, :]
            for d1, d2 in steps:
                m = m + column_of(d1[j], tr, k) * d2
            if len(o.shape) == 2:
                o[row + j * 64 : row + j * 64 + 64, :] = m
            else:
                o[2 * g + j, 0:64, :] = m
                put_small(o.at[2 * g + j], Stats(s.n, [s.m1[j]], [s.s1[j]], s.m2, s.s2), CA)
        if len(o.shape) == 2:
            put_z_stats(o, o.shape[0] - 8, g, s)


def whole(shape):
    return pl.BlockSpec(shape, lambda i, tab: (0,) * len(shape))


def call(kernel, tab, operands, outs, name, scratch=()):
    return pl.pallas_call(
        kernel,
        out_shape=tuple(jax.ShapeDtypeStruct(o, F32) for o in outs),
        grid_spec=pltpu.PrefetchScalarGridSpec(
            num_scalar_prefetch=1,
            grid=(1,),
            in_specs=[s for _, s in operands],
            out_specs=[whole(o) for o in outs],
            scratch_shapes=list(scratch) + [pltpu.VMEM((128, 128), F32)],
        ),
        compiler_params=pltpu.CompilerParams(vmem_limit_bytes=48 * 2**20),
        name=name,
    )(tab, *(a for a, _ in operands))


def part(t):
    for c, (first, last) in enumerate(CALLS):
        if first <= t < last:
            return c, t - first


def a_step(tab, own, peer, st, pst, d, received, plan, outs, name):
    c, i = part(AT[d % 8])
    spec = pl.BlockSpec((1, 264, CA), lambda _, tab: (i, 0, 0))
    operands = [(own[c], spec), (peer[c], spec), (st, whole((8, COLS))), (pst, whole((8, COLS)))]
    operands += [(r, whole(r.shape)) for r in received]
    plan = dict(plan, **{"in": len(received)})
    return call(functools.partial(a_kernel, plan), tab, operands, outs, name)


def y_place(i):
    per = CB // 128
    return i // per, i % per


def y_stats(ref, base, g):
    m1 = []
    for j in range(4):
        row, at = y_place(4 * g + j)
        m1.append(lanes(ref, base + row, at))
    return Stats(
        ref[base + 7 : base + 8, g * 128 : g * 128 + 1],
        m1,
        None,
        ref[base + MB + g : base + MB + 1 + g, :],
        ref[base + MB + 2 + g : base + MB + 3 + g, :],
    )


def put_y_stats(ref, base, g, s):
    for j in range(4):
        row, at = y_place(4 * g + j)
        ref[base + row : base + row + 1, at * 128 : at * 128 + 128] = s.m1[j]
    ref[base + MB + g : base + MB + 1 + g, :] = s.m2
    ref[base + MB + 2 + g : base + MB + 3 + g, :] = s.s2
    ref[base + 7 : base + 8, g * 128 : g * 128 + 128] = jnp.broadcast_to(s.n, (1, 128))


def b_kernel(plan, tab, *refs):
    parts = len(CALLS)
    own, peer = refs[:parts], refs[parts : 2 * parts]
    own_st, peer_st = refs[2 * parts : 3 * parts], refs[3 * parts : 4 * parts]
    st, pst = refs[4 * parts : 4 * parts + 2]
    rest = refs[4 * parts + 2 :]
    received, outs, tr = rest[: plan["in"]], rest[plan["in"] : -1], rest[-1]
    k = tab[2]
    dy = plan["dy"] % 4
    for o in outs:
        if len(o.shape) == 2:
            base = o.shape[0] - 8
            o[base : base + 8, :] = jnp.zeros((8, CB), F32)
    for g, (froms, out, row) in enumerate(plan["groups"]):
        both = []
        for sts, s2 in ((own_st, st), (peer_st, pst)):
            m1 = []
            for j in range(4):
                c, i = part(4 * g + j)
                m1.append(sts[c][i, 0:1, dy * 128 : dy * 128 + 128])
            both.append(Stats(s2[2:3, 0:1], m1, None, s2[0:1, CA:COLS], s2[1:2, CA:COLS]))
        s, d1, d2 = merge_stats(*both)
        steps = [(d1, d2)]
        for r in froms:
            s, d1, d2 = merge_stats(s, y_stats(received[r], received[r].shape[0] - 8, g))
            steps.append((d1, d2))
        o = outs[out]
        for j in range(4):
            c, i = part(4 * g + j)
            m = own[c][i, 0] + peer[c][i, 0]
            for r in froms:
                short = received[r].shape[0] == 264
                src = (j if short else 4 * g + j) * 64
                m = m + received[r][src : src + 64, :]
            for d1, d2 in steps:
                m = m + column_of(d1[j], tr, k) * d2
            if len(o.shape) == 2:
                o[row + j * 64 : row + j * 64 + 64, :] = m
            else:
                o[4 * g + j, 0:64, :] = m
                put_small(o.at[4 * g + j], Stats(s.n, [s.m1[j]], None, s.m2, s.s2), CB)
        if len(o.shape) == 2:
            put_y_stats(o, o.shape[0] - 8, g, s)


def b_step(tab, own_b, peer_b, own_a, peer_a, st, pst, dy, received, plan, outs, name):
    operands = []
    for arrays in (own_b, peer_b):
        for a in arrays:
            operands.append(
                (a, pl.BlockSpec((a.shape[0], 1, 64, CB), lambda _, tab: (0, dy % 4, 0, 0)))
            )
    for arrays in (own_a, peer_a):
        for a in arrays:
            operands.append((a, pl.BlockSpec((a.shape[0], 8, CA), lambda _, tab: (0, 32, 0))))
    operands += [(st, whole((8, COLS))), (pst, whole((8, COLS)))]
    operands += [(r, whole(r.shape)) for r in received]
    plan = dict(plan, **{"in": len(received), "dy": dy})
    return call(functools.partial(b_kernel, plan), tab, operands, outs, name)


def merge_small(refs, tr, k):
    s = small_stats(refs[0])
    m = refs[0][0:64, :]
    for r in refs[1:]:
        s, d1, d2 = merge_stats(s, small_stats(r))
        m = m + r[0:64, :] + column_of(d1[0], tr, k) * d2
    return s, m


def small_kernel(tab, local, received, out, tr):
    s, m = merge_small((local.at[0], received), tr, tab[2])
    out[0:64, :] = m
    put_small(out, s, CB)


def one_of(stack, i):
    shape = (1, *stack.shape[1:])
    return (stack, pl.BlockSpec(shape, lambda _, tab: (i, 0, 0)))


def small_step(tab, stack, d, received, name):
    operands = [one_of(stack, AT[d % 8]), (received, whole(received.shape))]
    return call(small_kernel, tab, operands, [(72, CB)], name)[0]


def final_kernel(tab, a0, a1, a2, a3, b0, b1, b2, out, loss, tr):
    k = tab[2]
    row0 = tab[4] + lax.broadcasted_iota(jnp.int32, (64, 1), 0)
    col0 = tab[5]
    sa, ma = merge_small((a0.at[0], a1, a2, a3), tr, k)
    sb, mb = merge_small((b0.at[0], b1, b2), tr, k)
    scale_rows = column_of(jnp.sqrt(sa.s1[0] / sa.n + EPS) * sa.n, tr, k)
    total = jnp.zeros((64, 128), F32)
    for m, s, at, width in ((ma, sa, 0, CA), (mb, sb, CA, CB)):
        scale_cols = jnp.sqrt(s.s2 / s.n + EPS)
        c = m / (scale_rows * scale_cols)
        out[:, at : at + width] = c
        cols = col0 + at + lax.broadcasted_iota(jnp.int32, (1, width), 1)
        off = 1.0 - c
        t = jnp.where(row0 == cols, off * off, OFF * (c * c))
        for i in range(0, width, 128):
            total = total + t[:, i : i + 128]
    total = jnp.sum(jnp.sum(total, axis=0, keepdims=True), axis=1, keepdims=True)
    loss[...] = jnp.broadcast_to(total, (8, 128))


def shift(size, by):
    return [(i, (i + by) % size) for i in range(size)]


def flip(size, by):
    return [(i, i ^ by) for i in range(size)]


def per_device(view_first, view_second, valid_rows):
    z, y, k, x = (lax.axis_index(a) for a in ("z", "y", "k", "col"))
    i = lax.iota(jnp.int32, 16)
    tab = jnp.where(i == 0, z, jnp.where(i == 1, y, jnp.where(i == 2, k, valid_rows[0])))
    tab = jnp.where(i == 4, 64 * (z * 8 + y * 2 + k), jnp.where(i == 5, x * COLS, tab))
    j = i - 8
    order = jnp.where(j == 7, 0, jnp.where(j % 2 == 1, 4 - (j + 1) // 2, 4 + j // 2))
    tab = jnp.where(i >= 8, (z + order) % 8, tab)

    c2, st = second_view(tab, view_second)
    swap = flip(2, 1)
    pst = lax.ppermute(st, "k", swap)
    own_a, peer_a, own_b, peer_b = [], [], [], []
    for first, last in CALLS:
        oa, ta, ob, tb = tiles(tab, view_first, c2, first, last)
        own_a.append(oa)
        own_b.append(ob)
        peer_a.append(lax.ppermute(ta, "k", swap))
        peer_b.append(lax.ppermute(tb, "k", swap))

    def a(d, received, groups, outs, name):
        return a_step(tab, own_a, peer_a, st, pst, d, received, {"groups": groups}, outs, name)

    def b(dy, received, groups, outs, name):
        return b_step(
            tab, own_b, peer_b, own_a, peer_a, st, pst, dy, received, {"groups": groups}, outs, name
        )

    up_z, down_z, up_y, down_y = shift(8, 1), shift(8, -1), shift(4, 1), shift(4, -1)
    long_a, half_a = (264, CA), (136, CA)
    up, down = a(4, [], [([], 0, 0), ([], 1, 0)], [half_a, half_a], "a4")
    up, down = lax.ppermute(up, "z", up_z), lax.ppermute(down, "z", down_z)
    up = a(3, [up], [([0], 0, 0), ([], 0, 128)], [long_a], "a3")[0]
    down = a(-3, [down], [([], 0, 0), ([0], 0, 128)], [long_a], "a5")[0]
    up, down = lax.ppermute(up, "z", up_z), lax.ppermute(down, "z", down_z)

    long_b, half_b = (520, CB), (264, CB)
    bup, bdown = b(2, [], [([], 0, 0), ([], 1, 0)], [half_b, half_b], "b2")
    bup, bdown = lax.ppermute(bup, "y", up_y), lax.ppermute(bdown, "y", down_y)

    for d in (2, 1):
        up = a(d, [up], [([0], 0, 0), ([0], 0, 128)], [long_a], f"a{d}")[0]
        down = a(-d, [down], [([0], 0, 0), ([0], 0, 128)], [long_a], f"a{8 - d}")[0]
        up, down = lax.ppermute(up, "z", up_z), lax.ppermute(down, "z", down_z)
        if d == 2:
            bup = b(1, [bup], [([0], 0, 0), ([], 0, 256)], [long_b], "b1")[0]
            bdown = b(-1, [bdown], [([], 0, 0), ([0], 0, 256)], [long_b], "b3")[0]
            bup, bdown = lax.ppermute(bup, "y", up_y), lax.ppermute(bdown, "y", down_y)
    a_rows = a(0, [up, down], [([0, 1], 0, 0), ([0, 1], 0, 0)], [(4, 72, CA)], "a0")[0]
    a_in = [lax.ppermute(a_rows[s], "y", shift(4, s)) for s in (1, 3, 2)]

    b_rows = b(0, [bup, bdown], [([0, 1], 0, 0), ([0, 1], 0, 0)], [(8, 72, CB)], "b0")[0]
    up = lax.ppermute(b_rows[AT[4]], "z", up_z)
    down = lax.ppermute(b_rows[AT[5]], "z", down_z)
    for d in (3, 2, 1):
        up = lax.ppermute(small_step(tab, b_rows, d, up, f"s{d}"), "z", up_z)
        if d < 3:
            down = lax.ppermute(small_step(tab, b_rows, -d, down, f"s{8 - d}"), "z", down_z)

    operands = [one_of(a_rows, 0)] + [(r, whole(r.shape)) for r in a_in]
    operands += [one_of(b_rows, AT[0]), (up, whole((72, CB))), (down, whole((72, CB)))]
    correlation, loss = call(final_kernel, tab, operands, [(64, COLS), (8, 128)], "final")
    for axis, by in (("k", 1), ("col", 1), ("col", 2), ("y", 1), ("y", 2), ("z", 1), ("z", 2), ("z", 4)):
        loss = loss + lax.ppermute(loss, axis, flip(lax.axis_size(axis), by))
    return correlation, loss[0, 0] / FEAT


def solution(mesh):
    finer = Mesh(mesh.devices.reshape(8, 4, 2, mesh.shape["col"]), ("z", "y", "k", "col"))
    dp = ("z", "y", "k")
    return jax.shard_map(
        per_device,
        mesh=finer,
        in_specs=(P(dp, None), P(dp, "col"), P(dp)),
        out_specs=(P(dp, "col"), P()),
        check_vma=False,
    )
```
